512 devices in a mesh: group: 2 (over y), ctx: 64 (over z, core), head: 4 (over x).
Axes of the slice: x: 4, y: 2, z: 32, core: 2. Of those that a mesh axis runs over, the one named last changes fastest.
The devices are a block of a 4x8x32 slice.
Arguments:
- query_nope: bfloat16 [8192, 8192], P(('group', 'ctx'), 'head'), parts along dimension 0, may hold values from -6 to 6
- query_rope: bfloat16 [8192, 4096], P(('group', 'ctx'), 'head'), parts along dimension 0, may hold values from -16 to 16
- kv_latent: bfloat16 [8192, 512], P(('group', 'ctx'), 'head'), parts along dimension 0, may hold values from -1300 to 1300
- key_rope: bfloat16 [8192, 64], P(('group', 'ctx')), parts along dimension 0, may hold values from -16 to 16
- latent_gain: float32 [512], replicated, may hold values from 0.1 to 1.9
- w_key: bfloat16 [512, 8192], P(None, 'head'), may hold values from -0.25 to 0.25
- w_value: bfloat16 [512, 8192], P(None, 'head'), may hold values from -0.25 to 0.25
- block_order: int32 [256], P('group'), parts along dimension 0, may hold values from 0 to 127, as said below
Outputs:
- attention_out: bfloat16 [8192, 8192], P(('group', 'ctx'), 'head'), parts along dimension 0
The draws below stay inside these ranges and needn't reach their ends.
There are 2 independent parts, one for each index of `group`. The reference program is written for one: setup_inputs(seed, part) draws one part's arguments, and reference() takes and returns one part's arrays. A program takes and returns all parts, laid end to end along the dimension named above; an argument that names none is the same for every part. Nothing has to cross between parts.
Inputs may be any that keep to these rules, and one draw needn't show every extreme that they name: `block_order`: A permutation of 0 to 127. Entries 2 c and 2 c + 1, for each c < 64, add up to 127.
All inputs are finite; a program needn't handle non-finite values.
Results may differ from the reference program's by a relative error of at most 0.0081.
Values may be sent and summed in bfloat16 or wider, within the bound.
A program may use at most 64 MiB of HBM per device.

```python
import jax
import jax.numpy as jnp
from jax import lax

LATENT = 512
ROPE = 64
NOPE = 128
VALUE_DIM = 128
HEADS = 64
TOK_DEV = 64
TOKENS = 4096
BLOCK = 32


def draw_query_rope(key, part):
    values = jnp.clip(jax.random.normal(jax.random.fold_in(key, 22), (TOKENS, HEADS, ROPE), jnp.float32), -6.0, 6.0)
    return values.reshape(TOKENS, HEADS * ROPE).astype(jnp.bfloat16)


def draw_key_rope(key, part):
    values = jnp.clip(jax.random.normal(jax.random.fold_in(key, 32), (TOKENS, ROPE), jnp.float32), -6.0, 6.0)
    return values.astype(jnp.bfloat16)


def draw_kv_latent(key, part):
    row_scale = jnp.exp(jax.random.uniform(jax.random.fold_in(key, 41), (TOKENS, 1), jnp.float32, 0.0, jnp.log(10.0)))
    column_scale = jnp.exp(jax.random.uniform(jax.random.fold_in(key, 42), (1, LATENT), jnp.float32, 0.0, jnp.log(10.0)))
    column_scale = column_scale * jnp.exp(jnp.log(3.0) * jnp.arange(LATENT, dtype=jnp.float32)[None, :] / LATENT)
    noise = jnp.clip(jax.random.normal(jax.random.fold_in(key, 45), (TOKENS, LATENT), jnp.float32), -4.0, 4.0)
    return (noise * row_scale * column_scale).astype(jnp.bfloat16)


def draw_block_order(key, part):
    devices = TOKENS // TOK_DEV
    blocks = 2 * devices
    shuffled = jax.random.permutation(jax.random.fold_in(key, 51), devices).astype(jnp.int32)
    flipped = jax.random.randint(jax.random.fold_in(key, 52), (devices,), 0, 2).astype(jnp.int32)
    early = jnp.where(flipped == 1, blocks - 1 - shuffled, shuffled)
    late = blocks - 1 - early
    return jnp.stack([early, late], 1).reshape(blocks).astype(jnp.int32)


def block_scale(key, extent, shards, smallest, top_value):
    def one(axis_at, blocks):
        steps = jax.random.uniform(jax.random.fold_in(jax.random.fold_in(key, 6), axis_at), (blocks,), jnp.float32, smallest / len(shards), top_value / len(shards))
        return jnp.repeat(jnp.exp(steps), extent[axis_at] // blocks).reshape((-1,) + (1,) * (len(extent) - axis_at - 1))

    factor_of = one(*shards[0])
    for cut in shards[1:]:
        factor_of = factor_of * one(*cut)
    return factor_of


def scatter_about(rng, extent, deviation, bound, shards=(), kind=jnp.bfloat16):
    result = jax.random.normal(rng, extent, jnp.float32) * deviation
    if len(shards) > 0:
        result = block_scale(rng, extent, shards, -0.22, 0.18) * result
    return jnp.clip(result, min=-bound, max=bound).astype(kind)


def setup_inputs(seed: int = 0, part: int = 0) -> dict:
    arg_keys = jax.random.split(jax.random.key(seed), 9)
    part_splits = jax.random.split(jax.random.fold_in(arg_keys[8], part), 9)
    return {
        "query_nope": scatter_about(part_splits[0], (TOKENS, HEADS * NOPE), 1.0, 6.0, ((0, 64), (1, 4))),
        "query_rope": draw_query_rope(jax.random.fold_in(jax.random.fold_in(arg_keys[8], part), 71), part),
        "kv_latent": draw_kv_latent(jax.random.fold_in(jax.random.fold_in(arg_keys[8], part), 71), part),
        "key_rope": draw_key_rope(jax.random.fold_in(jax.random.fold_in(arg_keys[8], part), 71), part),
        "latent_gain": jnp.clip(1.0 + 0.18 * jax.random.normal(arg_keys[4], (LATENT,), jnp.float32), 0.1, 1.9),
        "w_key": scatter_about(arg_keys[5], (LATENT, HEADS * NOPE), LATENT ** -0.5, 0.25, ((1, 4),)),
        "w_value": scatter_about(arg_keys[6], (LATENT, HEADS * VALUE_DIM), LATENT ** -0.5, 0.25, ((1, 4),)),
        "block_order": draw_block_order(jax.random.fold_in(jax.random.fold_in(arg_keys[8], part), 71), part),
    }


EPSILON = 1e-06

def rope_angle(positions, width):
    half_width = width // 2
    frequency = jnp.exp(-jnp.log(10000.0) * jnp.arange(half_width, dtype=jnp.float32) / half_width)
    return positions.astype(jnp.float32)[:, None] * frequency[None, :]

def rotate_pairs(values, angle):
    half_width = values.shape[-1] // 2
    first_half = values[..., :half_width]
    second = values[..., half_width:]
    cosine = jnp.cos(angle)
    sine_part = jnp.sin(angle)
    return jnp.concatenate([first_half * cosine - second * sine_part, second * cosine + first_half * sine_part], -1)

def reference(query_nope, query_rope, kv_latent, key_rope, latent_gain, w_key, w_value, block_order):
    row_ids = jnp.arange(TOKENS, dtype=jnp.int32)
    position = (block_order[row_ids // BLOCK] * BLOCK + row_ids % BLOCK).astype(jnp.int32)
    latent = kv_latent.astype(jnp.float32)
    mean_square = lax.optimization_barrier(jnp.mean(latent * latent, axis=1, keepdims=True))
    normed = (latent * lax.rsqrt(mean_square + EPSILON) * latent_gain[None, :]).astype(jnp.bfloat16)
    key_angle = rope_angle(position, ROPE)
    key_rotated = rotate_pairs(key_rope.astype(jnp.float32), key_angle).astype(jnp.bfloat16)
    query_rotated = rotate_pairs(query_rope.astype(jnp.float32).reshape(TOKENS, HEADS, ROPE), key_angle[:, None, :]).astype(jnp.bfloat16)
    nope_heads = jnp.transpose(query_nope.reshape(TOKENS, HEADS, NOPE), (1, 0, 2))
    rope_heads = jnp.transpose(query_rotated, (1, 0, 2))
    key_heads = jnp.transpose(w_key.reshape(LATENT, HEADS, NOPE), (1, 0, 2))
    value_heads = jnp.transpose(w_value.reshape(LATENT, HEADS, VALUE_DIM), (1, 0, 2))
    visible = position[None, :] <= position[:, None]
    score_scale = 1.0 / (NOPE + ROPE) ** 0.5

    def one_head(operands):
        nope_part, rope_part, key_map, value_map = operands
        absorbed = lax.dot_general(nope_part, key_map, (((1,), (1,)), ((), ())), preferred_element_type=jnp.float32).astype(jnp.bfloat16)
        scores = jnp.dot(absorbed, normed.T, preferred_element_type=jnp.float32)
        scores = (scores + jnp.dot(rope_part, key_rotated.T, preferred_element_type=jnp.float32)) * score_scale
        scores = jnp.where(visible, scores, -jnp.inf)
        row_max = lax.optimization_barrier(jnp.max(scores, axis=1, keepdims=True))
        exps = jnp.where(visible, jnp.exp(scores - row_max), 0.0)
        row_total = lax.optimization_barrier(jnp.sum(exps, axis=1, keepdims=True))
        mixed = (jnp.dot(exps.astype(jnp.bfloat16), normed, preferred_element_type=jnp.float32) / row_total).astype(jnp.bfloat16)
        return jnp.dot(mixed, value_map, preferred_element_type=jnp.float32)
    per_head = lax.map(one_head, (nope_heads, rope_heads, key_heads, value_heads))
    return jnp.transpose(per_head, (1, 0, 2)).reshape(TOKENS, HEADS * VALUE_DIM).astype(jnp.bfloat16)
```

```python
import functools
import math

import jax
import jax.numpy as jnp
from jax import lax
from jax.experimental import pallas as pl
from jax.experimental.pallas import tpu as pltpu
from jax.sharding import PartitionSpec as P

ROPE = 64
NOPE = 128
VALUE_DIM = 128
EPSILON = 1e-06
NEGATIVE = -1e30
LANES = 128
TILE = 256
NT = (((1,), (1,)), ((), ()))
SCORE_SCALE = math.log2(math.e) / math.sqrt(NOPE + ROPE)


def rotate_rows(values, position):
    lane = lax.broadcasted_iota(jnp.int32, values.shape, 1)
    half = ROPE // 2
    index = lax.rem(lane, half).astype(jnp.float32)
    angle = position.astype(jnp.float32) * jnp.exp(-math.log(10000.0) * index / half)
    low = lax.rem(lane, ROPE) < half
    partner = jnp.where(
        low, pltpu.roll(values, LANES - half, 1), pltpu.roll(values, half, 1)
    )
    sine = jnp.sin(angle)
    return values * jnp.cos(angle) + partner * jnp.where(low, -sine, sine)


def attend_kernel(
    heads,
    order_ref,
    q_nope_ref,
    q_rope_ref,
    w_key_hbm,
    w_value_hbm,
    keys_hbm,
    out_ref,
    w_key,
    w_value,
    keys,
    queries,
    scores,
    total_max,
    total_sum,
    mixed,
    key_sem,
    weight_sem,
):
    tokens, block = q_nope_ref.shape[0], q_nope_ref.shape[0] // 2
    latent = w_key.shape[0]
    rows = heads * block
    blocks = order_ref.shape[0]
    load_w_key = pltpu.make_async_copy(w_key_hbm, w_key, weight_sem.at[0])
    load_w_value = pltpu.make_async_copy(w_value_hbm, w_value, weight_sem.at[1])
    load_w_key.start()

    def load_block(row_block, carry):
        place = order_ref[row_block]
        pltpu.make_async_copy(
            keys_hbm.at[pl.ds(pl.multiple_of(row_block * block, block), block)],
            keys.at[pl.ds(pl.multiple_of(place * block, block), block)],
            key_sem,
        ).start()
        return carry

    lax.fori_loop(0, blocks, load_block, 0)
    load_w_value.start()

    here = lax.axis_index("ctx")
    places = (order_ref[2 * here], order_ref[2 * here + 1])
    row = lax.broadcasted_iota(jnp.int32, (tokens, LANES), 0)
    position = jnp.where(
        row < block, places[0] * block + row, places[1] * block + row - block
    )
    lane = lax.broadcasted_iota(jnp.int32, (tokens, LANES), 1)
    for pair in range(heads // 2):
        turned = rotate_rows(
            q_rope_ref[:, pair * LANES : (pair + 1) * LANES].astype(jnp.float32), position
        )
        turned = turned * SCORE_SCALE
        for side in range(2):
            head = 2 * pair + side
            alone = turned if side == 0 else pltpu.roll(turned, ROPE, 1)
            alone = jnp.where(lane < ROPE, alone, 0.0).astype(jnp.bfloat16)
            for member in range(2):
                queries[pl.ds(member * rows + head * block, block), latent:] = alone[
                    member * block : (member + 1) * block
                ]
    load_w_key.wait()
    for head in range(heads):
        columns = slice(head * NOPE, (head + 1) * NOPE)
        absorbed = lax.dot_general(
            q_nope_ref[:, columns], w_key[:, columns], NT, preferred_element_type=jnp.float32
        )
        absorbed = (absorbed * SCORE_SCALE).astype(jnp.bfloat16)
        for member in range(2):
            queries[pl.ds(member * rows + head * block, block), :latent] = absorbed[
                member * block : (member + 1) * block
            ]
    total_max[...] = jnp.full_like(total_max, NEGATIVE)
    total_sum[...] = jnp.zeros_like(total_sum)
    mixed[...] = jnp.zeros_like(mixed)
    pltpu.make_async_copy(keys_hbm, keys, key_sem).wait()

    per_tile = TILE // block
    first_tiles = places[0] // per_tile + 1
    tiles = first_tiles + places[1] // per_tile + 1

    def tile_of(step):
        second = step >= first_tiles
        member = second.astype(jnp.int32)
        tile = jnp.where(second, step - first_tiles, step)
        return member, tile

    def score(step):
        member, tile = tile_of(step)
        return lax.dot_general(
            queries[pl.ds(pl.multiple_of(member * rows, rows), rows), :],
            keys[pl.ds(pl.multiple_of(tile * TILE, TILE), TILE), :],
            NT,
            preferred_element_type=jnp.float32,
        )

    shift = lax.broadcasted_iota(jnp.int32, (block, TILE), 1) - lax.broadcasted_iota(
        jnp.int32, (block, TILE), 0
    )
    scores[0] = score(0)

    def one_step(step, carry):
        now = lax.rem(step, 2)
        member, tile = tile_of(step)
        here_rows = pl.ds(pl.multiple_of(member * rows, rows), rows)
        ahead = jnp.minimum(step + 1, tiles - 1)
        scores[1 - now] = score(ahead)
        place = jnp.where(member == 1, places[1], places[0])
        bound = place * block - tile * TILE
        visible = jnp.broadcast_to((shift <= bound)[None], (heads, block, TILE)).reshape(rows, TILE)
        part = jnp.where(visible, scores[now], NEGATIVE)
        before = total_max[here_rows]
        after = jnp.maximum(before, jnp.max(part, axis=1, keepdims=True))
        exps = jnp.exp2(part - jnp.concatenate([after] * (TILE // LANES), 1))
        shrink = jnp.exp2(before - after)
        total_max[here_rows] = after
        sums = exps[:, :LANES]
        for piece in range(1, TILE // LANES):
            sums = sums + exps[:, piece * LANES : (piece + 1) * LANES]
        total_sum[here_rows] = total_sum[here_rows] * shrink + sums
        gained = jnp.dot(
            exps.astype(jnp.bfloat16),
            keys[pl.ds(pl.multiple_of(tile * TILE, TILE), TILE), :latent],
            preferred_element_type=jnp.float32,
        )
        mixed[here_rows] = (
            mixed[here_rows] * jnp.concatenate([shrink] * (latent // LANES), 1) + gained
        )
        return carry

    lax.fori_loop(0, tiles, one_step, 0)
    load_w_value.wait()
    for head in range(heads):
        parts = []
        for member in range(2):
            at = pl.ds(member * rows + head * block, block)
            inverse = 1.0 / jnp.sum(total_sum[at], axis=1, keepdims=True)
            parts.append((mixed[at] * inverse).astype(jnp.bfloat16))
        columns = slice(head * VALUE_DIM, (head + 1) * VALUE_DIM)
        out_ref[:, columns] = jnp.dot(
            jnp.concatenate(parts, 0), w_value[:, columns], preferred_element_type=jnp.float32
        ).astype(jnp.bfloat16)


def attend(block_order, query_nope, query_rope, w_key, w_value, keys):
    tokens = query_nope.shape[0]
    heads = w_key.shape[1] // NOPE
    latent = w_key.shape[0]
    width = keys.shape[1]
    vmem = pl.BlockSpec(memory_space=pltpu.VMEM)
    hbm = pl.BlockSpec(memory_space=pl.ANY)
    return pl.pallas_call(
        functools.partial(attend_kernel, heads),
        out_shape=jax.ShapeDtypeStruct((tokens, w_value.shape[1]), jnp.bfloat16),
        in_specs=[pl.BlockSpec(memory_space=pltpu.SMEM), vmem, vmem, hbm, hbm, hbm],
        out_specs=vmem,
        scratch_shapes=[
            pltpu.VMEM(w_key.shape, jnp.bfloat16),
            pltpu.VMEM(w_value.shape, jnp.bfloat16),
            pltpu.VMEM(keys.shape, jnp.bfloat16),
            pltpu.VMEM((tokens * heads, width), jnp.bfloat16),
            pltpu.VMEM((2, tokens * heads // 2, TILE), jnp.float32),
            pltpu.VMEM((tokens * heads, LANES), jnp.float32),
            pltpu.VMEM((tokens * heads, LANES), jnp.float32),
            pltpu.VMEM((tokens * heads, latent), jnp.float32),
            pltpu.SemaphoreType.DMA,
            pltpu.SemaphoreType.DMA((2,)),
        ],
        compiler_params=pltpu.CompilerParams(vmem_limit_bytes=56 * 1024 * 1024),
        name="attend",
    )(block_order, query_nope, query_rope, w_key, w_value, keys)


def per_device(
    query_nope, query_rope, kv_latent, key_rope, latent_gain, w_key, w_value, block_order
):
    tokens = query_nope.shape[0]
    latent = w_key.shape[0]
    block = tokens // 2
    columns = kv_latent.shape[1]
    order = lax.dynamic_slice_in_dim(block_order, 2 * lax.axis_index("ctx"), 2, 0)
    place = (order[:, None] * block + jnp.arange(block, dtype=jnp.int32)[None]).reshape(tokens)
    half = ROPE // 2
    frequency = jnp.exp(-jnp.log(10000.0) * jnp.arange(half, dtype=jnp.float32) / half)
    angle = place.astype(jnp.float32)[:, None] * frequency[None]
    low, high = jnp.split(key_rope.astype(jnp.float32), 2, 1)
    cosine, sine = jnp.cos(angle), jnp.sin(angle)
    turned = jnp.concatenate([low * cosine - high * sine, high * cosine + low * sine], 1)
    column_part = kv_latent.astype(jnp.float32)
    square = lax.psum(jnp.sum(column_part * column_part, axis=1), "head")
    gain_part = lax.dynamic_slice_in_dim(latent_gain, lax.axis_index("head") * columns, columns, 0)
    scaled = (
        column_part * lax.rsqrt(square / latent + EPSILON)[:, None] * gain_part[None, :]
    ).astype(jnp.bfloat16)
    normed = lax.all_gather(scaled, "head", axis=1, tiled=True)
    mine = jnp.concatenate(
        [normed, turned.astype(jnp.bfloat16), jnp.zeros((tokens, LANES - ROPE), jnp.bfloat16)], 1
    )
    keys = lax.all_gather(mine, "ctx", axis=0, tiled=True)
    return attend(block_order, query_nope, query_rope, w_key, w_value, keys)


def solution(mesh):
    return jax.shard_map(
        per_device,
        mesh=mesh,
        in_specs=(
            P(("group", "ctx"), "head"),
            P(("group", "ctx"), "head"),
            P(("group", "ctx"), "head"),
            P(("group", "ctx"), None),
            P(),
            P(None, "head"),
            P(None, "head"),
            P("group"),
        ),
        out_specs=P(("group", "ctx"), "head"),
        check_vma=False,
    )
```
